32 devices in a mesh: space: 8 (over y, x, core), tm: 4 (over z).
Axes of the slice: x: 2, y: 2, z: 4, core: 2. Of those that a mesh axis runs over, the one named last changes fastest.
Arguments:
- vectors: bfloat16 [4, 2, 3, 96, 4096], P('tm', None, None, None, 'space'), may hold values from -6 to 6
- momenta: int32 [2, 3], replicated, may hold values from -3 to 3
- offsets: int32 [8, 3], replicated, may hold values from 0 to 56, as said below
Outputs:
- elementals: float32 [4, 96, 2, 18432], P(None, 'space')
The draws below stay inside these ranges and needn't reach their ends.
Inputs may be any that keep to these rules, and one draw needn't show every extreme that they name: `offsets`: each row is the corner of one block of 8 x 8 x 8 sites of the 64^3 lattice: its first two coordinates are multiples of 8, its third a multiple of 8; no two rows name the same block, so the blocks never intersect.
All inputs are finite; a program needn't handle non-finite values.
Results may differ from the reference program's by a relative error of at most 0.0055.
Values may be sent and summed in bfloat16 or wider, within the bound.
A program may use at most 128 MiB of HBM per device.

```python
import math
import jax
import jax.numpy as jnp
from jax import lax

NVEC = 96
MOMENTA = 2
LAT = 64
BRICK = 8
BRICK_Z = 8
SITES_DEV = 512
SITES = 4096
BRICKS = 8
TIME = 4
N_SPACE = 8


def draw_offsets(key, part):
    across = LAT // BRICK
    along = LAT // BRICK_Z
    chosen = jax.random.permutation(key, across * across * along)[:BRICKS].astype(jnp.int32)
    first = chosen // (across * along)
    second = chosen // along % across
    third = chosen % along
    return jnp.stack([first * BRICK, second * BRICK, third * BRICK_Z], axis=1).astype(jnp.int32)


def place_ends(array, own_key, smallest, largest):
    longest = array.shape.index(max(array.shape))
    spots = []
    for shift in (0, 1):
        where = [jax.random.randint(jax.random.fold_in(own_key, axis), (), 0, length) for axis, length in enumerate(array.shape)]
        where[longest] = (where[longest] + shift) % array.shape[longest]
        spots.append(tuple(where))
    return array.at[spots[0]].set(smallest).at[spots[1]].set(largest)


def level_of(own_key, extent, shards, low, high):
    loudness = 1.0
    for position, parts in shards:
        heights = jax.random.uniform(jax.random.fold_in(jax.random.fold_in(own_key, 6), position), (parts,), jnp.float32, low / len(shards), high / len(shards))
        loudness = loudness * jnp.repeat(jnp.exp(heights), extent[position] // parts).reshape((-1,) + (1,) * (len(extent) - 1 - position))
    return loudness


def bell_draw(own_key, extent, scale, reach, pieces=(), kind=jnp.bfloat16):
    result = jax.random.normal(own_key, extent, jnp.float32) * scale
    if len(pieces) > 0:
        result = level_of(own_key, extent, pieces, -0.22, 0.18) * result
    return jnp.clip(result, min=-reach, max=reach).astype(kind)


def setup_inputs(seed: int = 0) -> dict:
    arg_keys = jax.random.split(jax.random.key(seed), 4)
    return {
        "vectors": bell_draw(arg_keys[0], (TIME, 2, 3, NVEC, SITES), 1.0, 6.0, ((0, 4), (4, 8))),
        "momenta": place_ends(jax.random.randint(arg_keys[1], (MOMENTA, 3), -3, 4), jax.random.fold_in(arg_keys[1], 1), -3, 3).astype(jnp.int32),
        "offsets": draw_offsets(jax.random.fold_in(arg_keys[3], 71), 0),
    }


def local_coords(site):
    return jnp.stack([site // (BRICK * BRICK_Z), site // BRICK_Z % BRICK, site % BRICK_Z])

def phases(momenta, coords):
    product = lax.optimization_barrier(jnp.sum(momenta[:, :, None] * coords[None, :, :], axis=1))
    angle = (product % LAT).astype(jnp.float32) * (2.0 * math.pi / LAT)
    return jnp.stack([jnp.cos(angle), jnp.sin(angle)], axis=1).astype(jnp.float32)

def complex_term(w_real, w_imag, v_real, v_imag):
    return (w_real * v_real - w_imag * v_imag, w_real * v_imag + w_imag * v_real)

def cross_rows(phase, row_vecs, vecs):
    phase_f = phase.astype(jnp.float32)
    rows_f = row_vecs.astype(jnp.float32)
    cosine = phase_f[:, 0][:, None, None, :]
    sine = phase_f[:, 1][:, None, None, :]
    real_w = cosine * rows_f[0][None] - sine * rows_f[1][None]
    imag_w = cosine * rows_f[1][None] + sine * rows_f[0][None]
    real_w = jnp.transpose(real_w, (2, 0, 1, 3))
    imag_w = jnp.transpose(imag_w, (2, 0, 1, 3))
    real_v = vecs[0].astype(jnp.float32)
    imag_v = vecs[1].astype(jnp.float32)
    real_parts = []
    imag_parts = []
    for colour in range(3):
        first = (colour + 1) % 3
        second = (colour + 2) % 3
        plus_re, plus_im = complex_term(real_w[:, :, first, None, :], imag_w[:, :, first, None, :], real_v[second][None, None], imag_v[second][None, None])
        minus_re, minus_im = complex_term(real_w[:, :, second, None, :], imag_w[:, :, second, None, :], real_v[first][None, None], imag_v[first][None, None])
        real_parts.append(plus_re - minus_re)
        imag_parts.append(plus_im - minus_im)
    stacked = jnp.stack([jnp.stack(real_parts, axis=3), jnp.stack(imag_parts, axis=3)], axis=3)
    return stacked.astype(jnp.bfloat16)

def mixing(vecs):
    real_v = vecs[0]
    imag_v = vecs[1]
    return jnp.stack([jnp.stack([real_v, imag_v], axis=1), jnp.stack([-imag_v, real_v], axis=1)])

def reference(vectors, momenta, offsets):
    site = jnp.arange(SITES, dtype=jnp.int32)
    brick_of = site // SITES_DEV
    coords = local_coords(site % SITES_DEV) + jnp.transpose(offsets[brick_of])
    phase = phases(momenta, coords)
    rows = NVEC // N_SPACE
    scale = 1.0 / math.sqrt(SITES)

    def one_time(slab):

        def one_block(index):
            first_row = index * rows

            def add(total, shard):
                begin = shard * SITES_DEV
                phase_part = lax.dynamic_slice_in_dim(phase, begin, SITES_DEV, 2)
                vec_part = lax.dynamic_slice_in_dim(slab, begin, SITES_DEV, 3)
                row_vecs = lax.dynamic_slice_in_dim(vec_part, first_row, rows, 2)
                crossed = cross_rows(phase_part, row_vecs, vec_part).astype(jnp.float32)
                operand = mixing(vec_part).astype(jnp.float32)
                part = jnp.einsum('imjqcg,qcrkg->imjrk', crossed, operand, precision=lax.Precision.HIGHEST)
                return (total + part, None)
            empty = jnp.zeros((rows, MOMENTA, NVEC, 2, NVEC), jnp.float32)
            total, unused = lax.scan(add, empty, jnp.arange(N_SPACE, dtype=jnp.int32))
            return (total * scale).reshape(rows, MOMENTA, 2 * NVEC * NVEC)
        blocks = lax.map(one_block, jnp.arange(N_SPACE, dtype=jnp.int32))
        return blocks.reshape(NVEC, MOMENTA, 2 * NVEC * NVEC)
    return lax.map(one_time, vectors)
```

```python
import functools
import math

import jax
import jax.numpy as jnp
from jax import lax
from jax.experimental import pallas as pl
from jax.experimental.pallas import tpu as pltpu
from jax.sharding import PartitionSpec as P

LAT = 64
BRICK = 8
BRICK_Z = 8
JB = 32
LANES = 128


MESH = pl.DeviceIdType.MESH


def fill_phase(phase_ref, half, block, mom_ref, off_ref):
    sites = phase_ref.shape[2]
    moments = mom_ref.shape[0]
    site = lax.broadcasted_iota(jnp.int32, (1, sites), 1)
    coords = [site // (BRICK * BRICK_Z), site // BRICK_Z % BRICK, site % BRICK_Z]
    for p in range(moments):
        product = jnp.zeros((1, sites), jnp.int32)
        for axis in range(3):
            product = product + mom_ref[p, axis] * (coords[axis] + off_ref[block, axis])
        angle = (product % LAT).astype(jnp.float32) * (2.0 * math.pi / LAT)
        phase_ref[half, 2 * p : 2 * p + 1, :] = jnp.cos(angle)
        phase_ref[half, 2 * p + 1 : 2 * p + 2, :] = jnp.sin(angle)


def elementals_kernel(
    scale,
    chips,
    times,
    rows,
    mom_ref,
    off_ref,
    v_ref,
    z_ref,
    other_ref,
    phase_ref,
    rowf_ref,
    x_ref,
    lhs_a,
    lhs_b,
    acc_ref,
    own_ref,
    send_ref,
    take_ref,
    fin_ref,
    pair_sem,
    send_sem,
    take_sem,
    fin_sem,
    z_sem,
    up_sem,
    down_sem,
):
    nvec = v_ref.shape[2]
    sites = v_ref.shape[3]
    moments = mom_ref.shape[0]
    nblocks = nvec // JB
    group = 2 * moments * JB
    per_half = sites // LANES
    nchunks = 2 * per_half
    depth = 6 * LANES
    me = lax.axis_index("space")
    z = lax.axis_index("tm")
    core = lax.rem(me, 2)
    chip = me // 2
    mate = chip * 2 + 1 - core
    first = [sum((nblocks - m) * group for m in range(jb)) for jb in range(nblocks)]
    width = [(nblocks - jb) * group for jb in range(nblocks)]

    barrier = pltpu.get_barrier_semaphore()

    def greet(where):
        pl.semaphore_signal(barrier, inc=1, device_id=where, device_id_type=MESH)

    greet({"space": mate})
    for s in range(1, chips):
        greet({"space": lax.rem(chip + s, chips) * 2 + core})

    @pl.when(z > 0)
    def _():
        greet({"tm": z - 1})

    @pl.when(z < times - 1)
    def _():
        greet({"tm": z + 1})

    ends = jnp.minimum(z, 1) + jnp.minimum(times - 1 - z, 1)
    pl.semaphore_wait(barrier, chips + ends)

    pair = pltpu.make_async_remote_copy(
        src_ref=v_ref,
        dst_ref=other_ref,
        send_sem=pair_sem.at[0],
        recv_sem=pair_sem.at[1],
        device_id={"space": mate},
        device_id_type=MESH,
    )
    pair.start()
    fill_phase(phase_ref, 0, me, mom_ref, off_ref)
    fill_phase(phase_ref, 1, mate, mom_ref, off_ref)

    def prepare(half, source):
        def one(index, carry):
            lanes = pl.ds(pl.multiple_of(index * LANES, LANES), LANES)
            chunk = half * per_half + index
            for colour in range(3):
                real_v = source[0, colour, :, lanes].astype(jnp.float32)
                imag_v = source[1, colour, :, lanes].astype(jnp.float32)
                rowf_ref[chunk, colour] = real_v
                rowf_ref[chunk, 3 + colour] = imag_v
                for p in range(moments):
                    cosine = phase_ref[half, pl.ds(2 * p, 1), lanes]
                    sine = phase_ref[half, pl.ds(2 * p + 1, 1), lanes]
                    real_x = (cosine * real_v - sine * imag_v).astype(jnp.bfloat16)
                    imag_x = (cosine * imag_v + sine * real_v).astype(jnp.bfloat16)
                    table = ((real_x, -imag_x), (imag_x, real_x))
                    for r in range(2):
                        for part in range(2):
                            at = (colour * 2 + part) * LANES
                            for kb in range(nblocks):
                                base = kb * group + (2 * p + r) * JB
                                x_ref[chunk, base : base + JB, at : at + LANES] = table[r][part][
                                    kb * JB : (kb + 1) * JB
                                ]
            return carry

        lax.fori_loop(0, per_half, one, 0)

    prepare(0, v_ref)
    pair.wait()
    prepare(1, other_ref)

    def form(lhs, chunk, jb, row0):
        vecs = [
            [
                rowf_ref[chunk, part * 3 + colour, jb * JB : (jb + 1) * JB, :].astype(jnp.bfloat16)
                for colour in range(3)
            ]
            for part in range(2)
        ]
        for i in range(rows):
            row = [
                [
                    jnp.broadcast_to(
                        rowf_ref[chunk, part * 3 + colour, pl.ds(row0 + i, 1), :], (JB, LANES)
                    ).astype(jnp.bfloat16)
                    for colour in range(3)
                ]
                for part in range(2)
            ]
            for colour in range(3):
                a = (colour + 1) % 3
                b = (colour + 2) % 3
                real_d = (row[0][a] * vecs[0][b] - row[1][a] * vecs[1][b]) - (
                    row[0][b] * vecs[0][a] - row[1][b] * vecs[1][a]
                )
                imag_d = (row[0][a] * vecs[1][b] + row[1][a] * vecs[0][b]) - (
                    row[0][b] * vecs[1][a] + row[1][b] * vecs[0][a]
                )
                at = colour * 2 * LANES
                lhs[i * JB : (i + 1) * JB, at : at + LANES] = real_d
                lhs[i * JB : (i + 1) * JB, at + LANES : at + 2 * LANES] = imag_d

    def product(lhs, chunk, jb):
        return lax.dot_general(
            lhs[...],
            x_ref[chunk, jb * group :, :],
            (((1,), (1,)), ((), ())),
            preferred_element_type=jnp.float32,
        )

    def target(s):
        return lax.rem(chip + s + 1, chips)

    def forward(s, jb):
        cols = pl.ds(first[jb], width[jb])
        return pltpu.make_async_remote_copy(
            src_ref=send_ref.at[s, :, cols],
            dst_ref=take_ref.at[s, :, cols],
            send_sem=send_sem.at[jb, s],
            recv_sem=take_sem.at[jb, s],
            device_id={"space": target(s) * 2 + core},
            device_id_type=MESH,
        )

    def climb(t, jb):
        cols = pl.ds(first[jb], width[jb])
        return pltpu.make_async_remote_copy(
            src_ref=z_ref.at[t, :, cols],
            dst_ref=z_ref.at[t, :, cols],
            send_sem=up_sem.at[jb, t],
            recv_sem=z_sem.at[jb, t],
            device_id={"tm": z + 1},
            device_id_type=MESH,
        )

    def descend(t, jb):
        cols = pl.ds(first[jb], width[jb])
        return pltpu.make_async_remote_copy(
            src_ref=z_ref.at[t, :, cols],
            dst_ref=z_ref.at[t, :, cols],
            send_sem=down_sem.at[jb, t],
            recv_sem=z_sem.at[jb, t],
            device_id={"tm": z - 1},
            device_id_type=MESH,
        )

    def finish(jb):
        lo, hi = first[jb], first[jb] + width[jb]
        total = own_ref[:, lo:hi]
        for s in range(chips - 1):
            forward(s, jb).wait_recv()
            total = total + take_ref[s, :, lo:hi].astype(jnp.float32)
        z_ref[z, :, lo:hi] = (total * scale).astype(jnp.bfloat16)

        @pl.when(z < times - 1)
        def _():
            climb(z, jb).start()

        @pl.when(z > 0)
        def _():
            descend(z, jb).start()

    def relay(jb, dist):
        @pl.when(z - dist >= 0)
        def _():
            descend(z - dist, jb).wait_recv()

            @pl.when(z < times - 1)
            def _():
                climb(z - dist, jb).start()

        @pl.when(z + dist < times)
        def _():
            climb(z + dist, jb).wait_recv()

            @pl.when(z > 0)
            def _():
                descend(z + dist, jb).start()

    def run(jb, after):
        lo, hi = first[jb], first[jb] + width[jb]
        wide = width[jb]

        def one(s, carry):
            row0 = (target(s) * 2 + core) * rows
            form(lhs_a, 0, jb, row0)
            acc_ref[:, :wide] = jnp.zeros((rows * JB, wide), jnp.float32)

            def two(m, carry):
                form(lhs_b, 2 * m + 1, jb, row0)
                acc_ref[:, :wide] += product(lhs_a, 2 * m, jb)
                form(lhs_a, lax.rem(2 * m + 2, nchunks), jb, row0)
                acc_ref[:, :wide] += product(lhs_b, 2 * m + 1, jb)
                return carry

            lax.fori_loop(0, nchunks // 2, two, 0)

            @pl.when(s < chips - 1)
            def _():
                send_ref[s, :, lo:hi] = acc_ref[:, :wide].astype(jnp.bfloat16)
                forward(s, jb).start()

            @pl.when(s == chips - 1)
            def _():
                own_ref[:, lo:hi] = acc_ref[:, :wide]

            for when, act in after:

                @pl.when(s == when)
                def _():
                    act()

            return carry

        lax.fori_loop(0, chips, one, 0)

    order = list(range(nblocks - 1, -1, -1))
    for n, jb in enumerate(order):
        after = []
        if n >= 1:
            after.append((0, functools.partial(finish, order[n - 1])))
        if n >= 2:
            after.append((chips // 2, functools.partial(relay, order[n - 2], 1)))
        run(jb, after)
    for dist in range(2, times):
        for jb in order[:-2]:
            relay(jb, dist)
    if nblocks > 1:
        relay(order[-2], 1)
    finish(order[-1])
    if nblocks > 1:
        for dist in range(2, times):
            relay(order[-2], dist)
    for dist in range(1, times):
        relay(order[-1], dist)

    for jb in range(nblocks):
        for s in range(chips - 1):
            forward(s, jb).wait_send()
        for t in range(times):

            @pl.when((z < times - 1) & (t <= z))
            def _():
                climb(t, jb).wait_send()

            @pl.when((z > 0) & (t >= z))
            def _():
                descend(t, jb).wait_send()


def elementals(local, momenta, offsets):
    nvec = local.shape[2]
    sites = local.shape[3]
    groups = lax.axis_size("space")
    times = lax.axis_size("tm")
    chips = groups // 2
    rows = nvec // groups
    moments = momenta.shape[0]
    nblocks = nvec // JB
    group = 2 * moments * JB
    total = sum((nblocks - jb) * group for jb in range(nblocks))
    nchunks = 2 * sites // LANES
    depth = 6 * LANES
    tall = rows * JB
    scale = 1.0 / math.sqrt(sites * groups)
    dma = pltpu.SemaphoreType.DMA
    return pl.pallas_call(
        functools.partial(elementals_kernel, scale, chips, times, rows),
        out_shape=jax.ShapeDtypeStruct((times, tall, total), jnp.bfloat16),
        in_specs=[
            pl.BlockSpec(memory_space=pltpu.SMEM),
            pl.BlockSpec(memory_space=pltpu.SMEM),
            pl.BlockSpec(memory_space=pltpu.VMEM),
        ],
        out_specs=pl.BlockSpec(memory_space=pltpu.VMEM),
        scratch_shapes=[
            pltpu.VMEM((2, 3, nvec, sites), jnp.bfloat16),
            pltpu.VMEM((2, 2 * moments, sites), jnp.float32),
            pltpu.VMEM((nchunks, 6, nvec, LANES), jnp.float32),
            pltpu.VMEM((nchunks, nblocks * group, depth), jnp.bfloat16),
            pltpu.VMEM((tall, depth), jnp.bfloat16),
            pltpu.VMEM((tall, depth), jnp.bfloat16),
            pltpu.VMEM((tall, nblocks * group), jnp.float32),
            pltpu.VMEM((tall, total), jnp.float32),
            pltpu.VMEM((chips - 1, tall, total), jnp.bfloat16),
            pltpu.VMEM((chips - 1, tall, total), jnp.bfloat16),
            pltpu.VMEM((8, LANES), jnp.float32),
            dma((2,)),
            dma((nblocks, chips - 1)),
            dma((nblocks, chips - 1)),
            dma((2,)),
            dma((nblocks, times)),
            dma((nblocks, times)),
            dma((nblocks, times)),
        ],
        compiler_params=pltpu.CompilerParams(
            collective_id=0, has_side_effects=True, vmem_limit_bytes=60 * 1024 * 1024
        ),
        name="elementals",
    )(momenta, offsets, local)


def unpack_kernel(rows, moments, nvec, *refs):
    nblocks = nvec // JB
    group = 2 * moments * JB
    pack = LANES // JB
    source, out_ref, full = refs
    tall = full.shape[0] // (rows * moments)
    pieces = []
    at = 0
    for n in range(nblocks):
        for kb in range(n, nblocks):
            pieces.append((n, kb, at))
            at += group
    for jb, kb, at in pieces:
        for start in range(0, rows, pack):
            many = min(pack, rows - start)
            block = source[0, start * JB : (start + many) * JB, at : at + group].astype(
                jnp.float32
            )
            turned = -jnp.transpose(block) if jb != kb else None
            for n in range(many):
                for p in range(moments):
                    which = (start + n) * moments + p
                    for r in range(2):
                        lane = (2 * p + r) * JB
                        tile, spot = divmod(r * nvec + kb * JB, LANES)
                        full[
                            which * tall + tile, jb * JB : (jb + 1) * JB, spot : spot + JB
                        ] = block[n * JB : (n + 1) * JB, lane : lane + JB]
                        if jb != kb:
                            tile, spot = divmod(r * nvec + jb * JB, LANES)
                            full[
                                which * tall + tile, kb * JB : (kb + 1) * JB, spot : spot + JB
                            ] = turned[lane : lane + JB, n * JB : (n + 1) * JB]
    wide = 2 * nvec
    tiles = 2 * wide // LANES
    half = nvec // 2
    for which in range(rows * moments):
        parity = []
        for odd in range(2):
            for tile in range(tall):
                line = full[which * tall + tile, pl.ds(odd, half, stride=2), :]
                parity.append(line[:, : min(LANES, wide - tile * LANES)])
        both = jnp.concatenate(parity, axis=1)
        i, p = which // moments, which % moments
        base = i * half * tiles * moments
        for tile in range(tiles):
            out_ref[0, pl.ds(base + tile * moments + p, half, stride=tiles * moments), :] = both[
                :, tile * LANES : (tile + 1) * LANES
            ]


def unpack(packed, rows, moments, nvec):
    times = packed.shape[0]
    lines = nvec * nvec * 2 // LANES
    flat = pl.pallas_call(
        functools.partial(unpack_kernel, rows, moments, nvec),
        out_shape=jax.ShapeDtypeStruct((times, rows * lines * moments, LANES), jnp.float32),
        grid=(times,),
        in_specs=[
            pl.BlockSpec((1,) + packed.shape[1:], lambda t: (t, 0, 0)),
        ],
        out_specs=pl.BlockSpec((1, rows * lines * moments, LANES), lambda t: (t, 0, 0)),
        scratch_shapes=[
            pltpu.VMEM((rows * moments * -(-2 * nvec // LANES), nvec, LANES), jnp.float32)
        ],
        compiler_params=pltpu.CompilerParams(dimension_semantics=("arbitrary",)),
        name="unpack",
    )(packed)
    flat = flat.reshape(times, rows, lines, moments, LANES)
    return jnp.transpose(flat, (0, 1, 3, 2, 4)).reshape(times, rows, moments, lines * LANES)


def body(vectors, momenta, offsets):
    local = vectors[0]
    nvec = local.shape[2]
    rows = nvec // lax.axis_size("space")
    packed = elementals(local, momenta, offsets)
    return unpack(packed, rows, momenta.shape[0], nvec)


def solution(mesh):
    return jax.shard_map(
        body,
        mesh=mesh,
        in_specs=(P("tm", None, None, None, "space"), P(), P()),
        out_specs=P(None, "space", None, None),
        check_vma=False,
    )
```

```python
import functools
import math

import jax
import jax.numpy as jnp
from jax import lax
from jax.experimental import pallas as pl
from jax.experimental.pallas import tpu as pltpu
from jax.sharding import PartitionSpec as P

LAT = 64
BRICK = 8
BRICK_Z = 8
JB = 32
SPAN = 2
PARTS = 2
LAG = 1
HOP = 3
LANES = 128


MESH = pl.DeviceIdType.MESH


def fill_phase(phase_ref, half, block, mom_ref, off_ref):
    sites = phase_ref.shape[2]
    moments = mom_ref.shape[0]
    site = lax.broadcasted_iota(jnp.int32, (1, sites), 1)
    coords = [site // (BRICK * BRICK_Z), site // BRICK_Z % BRICK, site % BRICK_Z]
    for p in range(moments):
        product = jnp.zeros((1, sites), jnp.int32)
        for axis in range(3):
            product = product + mom_ref[p, axis] * (coords[axis] + off_ref[block, axis])
        angle = (product % LAT).astype(jnp.float32) * (2.0 * math.pi / LAT)
        phase_ref[half, 2 * p : 2 * p + 1, :] = jnp.cos(angle)
        phase_ref[half, 2 * p + 1 : 2 * p + 2, :] = jnp.sin(angle)


def elementals_kernel(
    scale,
    chips,
    times,
    rows,
    mom_ref,
    off_ref,
    v_ref,
    z_ref,
    other_ref,
    phase_ref,
    rowf_ref,
    x_ref,
    lhs_a,
    lhs_b,
    acc_ref,
    own_ref,
    send_ref,
    take_ref,
    pair_sem,
    send_sem,
    take_sem,
    z_sem,
    up_sem,
    down_sem,
):
    nvec = v_ref.shape[2]
    sites = v_ref.shape[3]
    moments = mom_ref.shape[0]
    nblocks = nvec // JB
    group = 2 * moments * JB
    per_half = sites // LANES
    nchunks = 2 * per_half
    depth = 6 * LANES
    me = lax.axis_index("space")
    z = lax.axis_index("tm")
    core = lax.rem(me, 2)
    chip = me // 2
    mate = chip * 2 + 1 - core
    reach = nblocks // 2 + 1
    wide = reach * group
    pieces = nblocks * chips
    share = rows * JB // PARTS
    steps = nchunks // SPAN

    barrier = pltpu.get_barrier_semaphore()

    def greet(where):
        pl.semaphore_signal(barrier, inc=1, device_id=where, device_id_type=MESH)

    greet({"space": mate})
    for s in range(1, chips):
        greet({"space": lax.rem(chip + s, chips) * 2 + core})

    @pl.when(z > 0)
    def _():
        greet({"tm": z - 1})

    @pl.when(z < times - 1)
    def _():
        greet({"tm": z + 1})

    fill_phase(phase_ref, 0, me, mom_ref, off_ref)
    fill_phase(phase_ref, 1, mate, mom_ref, off_ref)
    ends = jnp.minimum(z, 1) + jnp.minimum(times - 1 - z, 1)
    pl.semaphore_wait(barrier, chips + ends)

    pair = pltpu.make_async_remote_copy(
        src_ref=v_ref,
        dst_ref=other_ref,
        send_sem=pair_sem.at[0],
        recv_sem=pair_sem.at[1],
        device_id={"space": mate},
        device_id_type=MESH,
    )
    pair.start()

    def prepare(half, source):
        def one(index, carry):
            lanes = pl.ds(pl.multiple_of(index * LANES, LANES), LANES)
            chunk = half * per_half + index
            step = chunk // SPAN
            place = pl.multiple_of(lax.rem(chunk, SPAN) * depth, LANES)
            for colour in range(3):
                real_v = source[0, colour, :, lanes].astype(jnp.float32)
                imag_v = source[1, colour, :, lanes].astype(jnp.float32)
                rowf_ref[chunk, colour] = real_v
                rowf_ref[chunk, 3 + colour] = imag_v
                for p in range(moments):
                    cosine = phase_ref[half, pl.ds(2 * p, 1), lanes]
                    sine = phase_ref[half, pl.ds(2 * p + 1, 1), lanes]
                    real_x = (cosine * real_v - sine * imag_v).astype(jnp.bfloat16)
                    imag_x = (cosine * imag_v + sine * real_v).astype(jnp.bfloat16)
                    table = ((real_x, -imag_x), (imag_x, real_x))
                    for r in range(2):
                        for part in range(2):
                            at = (colour * 2 + part) * LANES
                            for n in range(nblocks + reach - 1):
                                kb = n % nblocks
                                base = n * group + (2 * p + r) * JB
                                x_ref[step, base : base + JB, pl.ds(place + at, LANES)] = table[r][
                                    part
                                ][kb * JB : (kb + 1) * JB]
            return carry

        lax.fori_loop(0, per_half, one, 0)

    prepare(0, v_ref)
    pair.wait()
    prepare(1, other_ref)

    def target(s):
        return lax.rem(chip + s + 1, chips)

    def form(lhs, piece, step):
        rows_j = pl.ds(pl.multiple_of(piece // chips * JB, JB), JB)
        row0 = (target(lax.rem(piece, chips)) * 2 + core) * rows
        for n in range(SPAN):
            chunk = step * SPAN + n
            vecs = [
                [
                    rowf_ref[chunk, part * 3 + colour, rows_j, :].astype(jnp.bfloat16)
                    for colour in range(3)
                ]
                for part in range(2)
            ]
            for i in range(rows):
                row = [
                    [
                        jnp.broadcast_to(
                            rowf_ref[chunk, part * 3 + colour, pl.ds(row0 + i, 1), :], (JB, LANES)
                        ).astype(jnp.bfloat16)
                        for colour in range(3)
                    ]
                    for part in range(2)
                ]
                for colour in range(3):
                    a = (colour + 1) % 3
                    b = (colour + 2) % 3
                    real_d = (row[0][a] * vecs[0][b] - row[1][a] * vecs[1][b]) - (
                        row[0][b] * vecs[0][a] - row[1][b] * vecs[1][a]
                    )
                    imag_d = (row[0][a] * vecs[1][b] + row[1][a] * vecs[0][b]) - (
                        row[0][b] * vecs[1][a] + row[1][b] * vecs[0][a]
                    )
                    at = n * depth + colour * 2 * LANES
                    lhs[i * JB : (i + 1) * JB, at : at + LANES] = real_d
                    lhs[i * JB : (i + 1) * JB, at + LANES : at + 2 * LANES] = imag_d

    def product(lhs, piece, step):
        rows_x = pl.ds(pl.multiple_of(piece // chips * group, group), wide)
        return lax.dot_general(
            lhs[...],
            x_ref[step, rows_x, :],
            (((1,), (1,)), ((), ())),
            preferred_element_type=jnp.float32,
        )

    def forward(s, jb):
        return pltpu.make_async_remote_copy(
            src_ref=send_ref.at[jb, s],
            dst_ref=take_ref.at[jb, s],
            send_sem=send_sem.at[jb, s],
            recv_sem=take_sem.at[jb, s],
            device_id={"space": target(s) * 2 + core},
            device_id_type=MESH,
        )

    def climb(t, unit):
        jb, part = divmod(unit, PARTS)
        block = pl.ds(part * share, share)
        return pltpu.make_async_remote_copy(
            src_ref=z_ref.at[t, jb, block],
            dst_ref=z_ref.at[t, jb, block],
            send_sem=up_sem.at[unit, t],
            recv_sem=z_sem.at[unit, t],
            device_id={"tm": z + 1},
            device_id_type=MESH,
        )

    def descend(t, unit):
        jb, part = divmod(unit, PARTS)
        block = pl.ds(part * share, share)
        return pltpu.make_async_remote_copy(
            src_ref=z_ref.at[t, jb, block],
            dst_ref=z_ref.at[t, jb, block],
            send_sem=down_sem.at[unit, t],
            recv_sem=z_sem.at[unit, t],
            device_id={"tm": z - 1},
            device_id_type=MESH,
        )

    def finish(jb):
        for s in range(chips - 1):
            forward(s, jb).wait_recv()
        for part in range(PARTS):
            lo, hi = part * share, (part + 1) * share
            total = own_ref[jb, lo:hi]
            for s in range(chips - 1):
                total = total + take_ref[jb, s, lo:hi].astype(jnp.float32)
            z_ref[z, jb, lo:hi] = (total * scale).astype(jnp.bfloat16)
            unit = jb * PARTS + part

            @pl.when(z < times - 1)
            def _():
                climb(z, unit).start()

            @pl.when(z > 0)
            def _():
                descend(z, unit).start()

    def relay(unit, dist):
        @pl.when(z - dist >= 0)
        def _():
            descend(z - dist, unit).wait_recv()

            @pl.when(z < times - 1)
            def _():
                climb(z - dist, unit).start()

        @pl.when(z + dist < times)
        def _():
            climb(z + dist, unit).wait_recv()

            @pl.when(z > 0)
            def _():
                descend(z + dist, unit).start()

    halves = steps // 2
    plan = {}
    tail = []
    events = []
    for jb in range(nblocks):
        begin = halves * chips * (jb + 1) + LAG
        events.append((begin, finish, (jb,)))
        for part in range(PARTS):
            for dist in range(1, times):
                at = begin + part + HOP * dist
                events.append((at, relay, (jb * PARTS + part, dist)))
    events.sort(key=lambda event: event[0])
    for at, act, operands in events:
        if at < halves * pieces:
            plan.setdefault(at, []).append((act, operands))
        else:
            tail.append((act, operands))

    def one(piece, carry):
        jb = piece // chips
        s = lax.rem(piece, chips)
        for step in range(0, steps, 2):
            form(lhs_b, piece, step + 1)
            first = product(lhs_a, piece, step)
            acc_ref[...] = first if step == 0 else acc_ref[...] + first
            if step + 2 < steps:
                form(lhs_a, piece, step + 2)
            else:
                form(lhs_a, lax.rem(piece + 1, pieces), 0)
            acc_ref[...] += product(lhs_b, piece, step + 1)
            for at, acts in plan.items():
                if at % halves == step // 2:

                    @pl.when(piece == at // halves)
                    def _():
                        for act, operands in acts:
                            act(*operands)

        @pl.when(s < chips - 1)
        def _():
            send_ref[jb, s] = acc_ref[...].astype(jnp.bfloat16)
            forward(s, jb).start()

        @pl.when(s == chips - 1)
        def _():
            own_ref[jb] = acc_ref[...]

        return carry

    form(lhs_a, 0, 0)
    lax.fori_loop(0, pieces, one, 0)
    for act, operands in tail:
        act(*operands)

    for jb in range(nblocks):
        for s in range(chips - 1):
            forward(s, jb).wait_send()
    for unit in range(nblocks * PARTS):
        for t in range(times):

            @pl.when((z < times - 1) & (t <= z))
            def _():
                climb(t, unit).wait_send()

            @pl.when((z > 0) & (t >= z))
            def _():
                descend(t, unit).wait_send()


def elementals(local, momenta, offsets):
    nvec = local.shape[2]
    sites = local.shape[3]
    groups = lax.axis_size("space")
    times = lax.axis_size("tm")
    chips = groups // 2
    rows = nvec // groups
    moments = momenta.shape[0]
    nblocks = nvec // JB
    group = 2 * moments * JB
    reach = nblocks // 2 + 1
    wide = reach * group
    nchunks = 2 * sites // LANES
    depth = 6 * LANES
    tall = rows * JB
    scale = 1.0 / math.sqrt(sites * groups)
    dma = pltpu.SemaphoreType.DMA
    return pl.pallas_call(
        functools.partial(elementals_kernel, scale, chips, times, rows),
        out_shape=jax.ShapeDtypeStruct((times, nblocks, tall, wide), jnp.bfloat16),
        in_specs=[
            pl.BlockSpec(memory_space=pltpu.SMEM),
            pl.BlockSpec(memory_space=pltpu.SMEM),
            pl.BlockSpec(memory_space=pltpu.VMEM),
        ],
        out_specs=pl.BlockSpec(memory_space=pltpu.VMEM),
        scratch_shapes=[
            pltpu.VMEM((2, 3, nvec, sites), jnp.bfloat16),
            pltpu.VMEM((2, 2 * moments, sites), jnp.float32),
            pltpu.VMEM((nchunks, 6, nvec, LANES), jnp.float32),
            pltpu.VMEM(
                (nchunks // SPAN, (nblocks + reach - 1) * group, SPAN * depth), jnp.bfloat16
            ),
            pltpu.VMEM((tall, SPAN * depth), jnp.bfloat16),
            pltpu.VMEM((tall, SPAN * depth), jnp.bfloat16),
            pltpu.VMEM((tall, wide), jnp.float32),
            pltpu.VMEM((nblocks, tall, wide), jnp.float32),
            pltpu.VMEM((nblocks, chips - 1, tall, wide), jnp.bfloat16),
            pltpu.VMEM((nblocks, chips - 1, tall, wide), jnp.bfloat16),
            dma((2,)),
            dma((nblocks, chips - 1)),
            dma((nblocks, chips - 1)),
            dma((nblocks * PARTS, times)),
            dma((nblocks * PARTS, times)),
            dma((nblocks * PARTS, times)),
        ],
        compiler_params=pltpu.CompilerParams(
            collective_id=0, has_side_effects=True, vmem_limit_bytes=60 * 1024 * 1024
        ),
        name="elementals",
    )(momenta, offsets, local)


def unpack_kernel(rows, moments, nvec, *refs):
    nblocks = nvec // JB
    group = 2 * moments * JB
    pack = LANES // JB
    source, out_ref, full = refs
    tall = full.shape[0] // (rows * moments)
    pieces = []
    for jb in range(nblocks):
        for d in range(nblocks // 2 + 1):
            pieces.append((jb, (jb + d) % nblocks, d * group))
    for jb, kb, at in pieces:
        for start in range(0, rows, pack):
            many = min(pack, rows - start)
            block = source[0, jb, start * JB : (start + many) * JB, at : at + group].astype(
                jnp.float32
            )
            turned = -jnp.transpose(block) if jb != kb else None
            for n in range(many):
                for p in range(moments):
                    which = (start + n) * moments + p
                    for r in range(2):
                        lane = (2 * p + r) * JB
                        tile, spot = divmod(r * nvec + kb * JB, LANES)
                        full[
                            which * tall + tile, jb * JB : (jb + 1) * JB, spot : spot + JB
                        ] = block[n * JB : (n + 1) * JB, lane : lane + JB]
                        if jb != kb:
                            tile, spot = divmod(r * nvec + jb * JB, LANES)
                            full[
                                which * tall + tile, kb * JB : (kb + 1) * JB, spot : spot + JB
                            ] = turned[lane : lane + JB, n * JB : (n + 1) * JB]
    wide = 2 * nvec
    tiles = 2 * wide // LANES
    half = nvec // 2
    for which in range(rows * moments):
        parity = []
        for odd in range(2):
            for tile in range(tall):
                line = full[which * tall + tile, pl.ds(odd, half, stride=2), :]
                parity.append(line[:, : min(LANES, wide - tile * LANES)])
        both = jnp.concatenate(parity, axis=1)
        i, p = which // moments, which % moments
        base = i * half * tiles * moments
        for tile in range(tiles):
            out_ref[0, pl.ds(base + tile * moments + p, half, stride=tiles * moments), :] = both[
                :, tile * LANES : (tile + 1) * LANES
            ]


def unpack(packed, rows, moments, nvec):
    times = packed.shape[0]
    lines = nvec * nvec * 2 // LANES
    flat = pl.pallas_call(
        functools.partial(unpack_kernel, rows, moments, nvec),
        out_shape=jax.ShapeDtypeStruct((times, rows * lines * moments, LANES), jnp.float32),
        grid=(times,),
        in_specs=[
            pl.BlockSpec((1,) + packed.shape[1:], lambda t: (t, 0, 0, 0)),
        ],
        out_specs=pl.BlockSpec((1, rows * lines * moments, LANES), lambda t: (t, 0, 0)),
        scratch_shapes=[
            pltpu.VMEM((rows * moments * -(-2 * nvec // LANES), nvec, LANES), jnp.float32)
        ],
        compiler_params=pltpu.CompilerParams(dimension_semantics=("arbitrary",)),
        name="unpack",
    )(packed)
    flat = flat.reshape(times, rows, lines, moments, LANES)
    return jnp.transpose(flat, (0, 1, 3, 2, 4)).reshape(times, rows, moments, lines * LANES)


def body(vectors, momenta, offsets):
    local = vectors[0]
    nvec = local.shape[2]
    rows = nvec // lax.axis_size("space")
    packed = elementals(local, momenta, offsets)
    return unpack(packed, rows, momenta.shape[0], nvec)


def solution(mesh):
    return jax.shard_map(
        body,
        mesh=mesh,
        in_specs=(P("tm", None, None, None, "space"), P(), P()),
        out_specs=P(None, "space", None, None),
        check_vma=False,
    )
```

```python
import functools
import math

import jax
import jax.numpy as jnp
from jax import lax
from jax.experimental import pallas as pl
from jax.experimental.pallas import tpu as pltpu
from jax.sharding import PartitionSpec as P

LAT = 64
BRICK = 8
BRICK_Z = 8
JB = 32
SPAN = 4
PARTS = 2
LAG = 1
HOP = 2
LANES = 128


MESH = pl.DeviceIdType.MESH


def fill_phase(phase_ref, half, block, mom_ref, off_ref):
    sites = phase_ref.shape[2]
    moments = mom_ref.shape[0]
    site = lax.broadcasted_iota(jnp.int32, (1, sites), 1)
    coords = [site // (BRICK * BRICK_Z), site // BRICK_Z % BRICK, site % BRICK_Z]
    for p in range(moments):
        product = jnp.zeros((1, sites), jnp.int32)
        for axis in range(3):
            product = product + mom_ref[p, axis] * (coords[axis] + off_ref[axis, block])
        angle = (product % LAT).astype(jnp.float32) * (2.0 * math.pi / LAT)
        phase_ref[half, 2 * p : 2 * p + 1, :] = jnp.cos(angle)
        phase_ref[half, 2 * p + 1 : 2 * p + 2, :] = jnp.sin(angle)


def spots(height, width):
    j = lax.broadcasted_iota(jnp.int32, (height, width), 0) % (JB // 2)
    k = lax.broadcasted_iota(jnp.int32, (height, width), 1) % JB
    return j, k


def folded(height, width):
    j, k = spots(height, width)
    return k > j


def elementals_kernel(
    scale,
    chips,
    times,
    rows,
    mom_ref,
    off_ref,
    v_ref,
    z_ref,
    other_ref,
    phase_ref,
    rowf_ref,
    x_ref,
    lhs_a,
    lhs_b,
    acc_ref,
    own_ref,
    send_ref,
    take_ref,
    pair_sem,
    send_sem,
    take_sem,
    z_sem,
    up_sem,
    down_sem,
):
    nvec = v_ref.shape[2]
    sites = v_ref.shape[3]
    moments = mom_ref.shape[0]
    nblocks = nvec // JB
    group = 2 * moments * JB
    per_half = sites // LANES
    nchunks = 2 * per_half
    depth = 6 * LANES
    me = lax.axis_index("space")
    z = lax.axis_index("tm")
    core = lax.rem(me, 2)
    chip = me // 2
    mate = chip * 2 + 1 - core
    reach = nblocks // 2 + 1
    wide = reach * group
    pieces = nblocks * chips
    share = rows * JB // PARTS
    slab = share * reach - share // 2
    steps = nchunks // SPAN

    barrier = pltpu.get_barrier_semaphore()

    def greet(where):
        pl.semaphore_signal(barrier, inc=1, device_id=where, device_id_type=MESH)

    greet({"space": mate})
    for s in range(1, chips):
        greet({"space": lax.rem(chip + s, chips) * 2 + core})

    @pl.when(z > 0)
    def _():
        greet({"tm": z - 1})

    @pl.when(z < times - 1)
    def _():
        greet({"tm": z + 1})

    fill_phase(phase_ref, 0, me, mom_ref, off_ref)
    fill_phase(phase_ref, 1, mate, mom_ref, off_ref)
    ends = jnp.minimum(z, 1) + jnp.minimum(times - 1 - z, 1)
    pl.semaphore_wait(barrier, chips + ends)

    pair = pltpu.make_async_remote_copy(
        src_ref=v_ref,
        dst_ref=other_ref,
        send_sem=pair_sem.at[0],
        recv_sem=pair_sem.at[1],
        device_id={"space": mate},
        device_id_type=MESH,
    )
    pair.start()

    def prepare(half, source):
        def one(index, carry):
            lanes = pl.ds(pl.multiple_of(index * LANES, LANES), LANES)
            chunk = half * per_half + index
            step = chunk // SPAN
            place = pl.multiple_of(lax.rem(chunk, SPAN) * depth, LANES)
            for colour in range(3):
                real_v = source[0, colour, :, lanes].astype(jnp.float32)
                imag_v = source[1, colour, :, lanes].astype(jnp.float32)
                rowf_ref[chunk, colour] = real_v
                rowf_ref[chunk, 3 + colour] = imag_v
                for p in range(moments):
                    cosine = phase_ref[half, pl.ds(2 * p, 1), lanes]
                    sine = phase_ref[half, pl.ds(2 * p + 1, 1), lanes]
                    real_x = (cosine * real_v - sine * imag_v).astype(jnp.bfloat16)
                    imag_x = (cosine * imag_v + sine * real_v).astype(jnp.bfloat16)
                    table = ((real_x, -imag_x), (imag_x, real_x))
                    for r in range(2):
                        for part in range(2):
                            at = (colour * 2 + part) * LANES
                            for n in range(nblocks + reach - 1):
                                kb = n % nblocks
                                base = n * group + (2 * p + r) * JB
                                x_ref[step, base : base + JB, pl.ds(place + at, LANES)] = table[r][
                                    part
                                ][kb * JB : (kb + 1) * JB]
            return carry

        lax.fori_loop(0, per_half, one, 0)

    prepare(0, v_ref)
    pair.wait()
    prepare(1, other_ref)

    def target(s):
        return lax.rem(chip + s + 1, chips)

    def form(lhs, piece, step):
        rows_j = pl.ds(pl.multiple_of(piece // chips * JB, JB), JB)
        row0 = (target(lax.rem(piece, chips)) * 2 + core) * rows
        for n in range(SPAN):
            chunk = step * SPAN + n
            vecs = [
                [
                    rowf_ref[chunk, part * 3 + colour, rows_j, :].astype(jnp.bfloat16)
                    for colour in range(3)
                ]
                for part in range(2)
            ]
            for i in range(rows):
                row = [
                    [
                        jnp.broadcast_to(
                            rowf_ref[chunk, part * 3 + colour, pl.ds(row0 + i, 1), :], (JB, LANES)
                        ).astype(jnp.bfloat16)
                        for colour in range(3)
                    ]
                    for part in range(2)
                ]
                for colour in range(3):
                    a = (colour + 1) % 3
                    b = (colour + 2) % 3
                    real_d = (row[0][a] * vecs[0][b] - row[1][a] * vecs[1][b]) - (
                        row[0][b] * vecs[0][a] - row[1][b] * vecs[1][a]
                    )
                    imag_d = (row[0][a] * vecs[1][b] + row[1][a] * vecs[0][b]) - (
                        row[0][b] * vecs[1][a] + row[1][b] * vecs[0][a]
                    )
                    at = n * depth + colour * 2 * LANES
                    lhs[i * JB : (i + 1) * JB, at : at + LANES] = real_d
                    lhs[i * JB : (i + 1) * JB, at + LANES : at + 2 * LANES] = imag_d

    def product(lhs, piece, step):
        rows_x = pl.ds(pl.multiple_of(piece // chips * group, group), wide)
        return lax.dot_general(
            lhs[...],
            x_ref[step, rows_x, :],
            (((1,), (1,)), ((), ())),
            preferred_element_type=jnp.float32,
        )

    def forward(s, jb):
        return pltpu.make_async_remote_copy(
            src_ref=send_ref.at[jb, s],
            dst_ref=take_ref.at[jb, s],
            send_sem=send_sem.at[jb, s],
            recv_sem=take_sem.at[jb, s],
            device_id={"space": target(s) * 2 + core},
            device_id_type=MESH,
        )

    def climb(t, unit):
        jb, part = divmod(unit, PARTS)
        block = pl.ds(part * slab, slab)
        return pltpu.make_async_remote_copy(
            src_ref=z_ref.at[t, jb, block],
            dst_ref=z_ref.at[t, jb, block],
            send_sem=up_sem.at[unit, t],
            recv_sem=z_sem.at[unit, t],
            device_id={"tm": z + 1},
            device_id_type=MESH,
        )

    def descend(t, unit):
        jb, part = divmod(unit, PARTS)
        block = pl.ds(part * slab, slab)
        return pltpu.make_async_remote_copy(
            src_ref=z_ref.at[t, jb, block],
            dst_ref=z_ref.at[t, jb, block],
            send_sem=down_sem.at[unit, t],
            recv_sem=z_sem.at[unit, t],
            device_id={"tm": z - 1},
            device_id_type=MESH,
        )

    def finish(jb):
        for s in range(chips - 1):
            forward(s, jb).wait_recv()
        for part in range(PARTS):
            lo, hi = part * share, (part + 1) * share
            total = own_ref[jb, lo:hi]
            for s in range(chips - 1):
                total = total + take_ref[jb, s, lo:hi].astype(jnp.float32)
            total = total * scale
            at = part * slab
            for d in range(1, reach):
                z_ref[z, jb, at : at + share] = total[:, d * group : (d + 1) * group].astype(
                    jnp.bfloat16
                )
                at += share
            square = total[:, :group].reshape(share // JB, JB, group)
            upper = square[:, : JB // 2].reshape(share // 2, group)
            lower = square[:, JB // 2 :].reshape(share // 2, group)
            keep = folded(share // 2, group)
            z_ref[z, jb, at : at + share // 2] = jnp.where(
                keep, upper, pltpu.roll(lower, group - JB // 2, 1)
            ).astype(jnp.bfloat16)
            unit = jb * PARTS + part

            @pl.when(z < times - 1)
            def _():
                climb(z, unit).start()

            @pl.when(z > 0)
            def _():
                descend(z, unit).start()

    def relay(unit, dist):
        @pl.when(z - dist >= 0)
        def _():
            descend(z - dist, unit).wait_recv()

            @pl.when(z < times - 1)
            def _():
                climb(z - dist, unit).start()

        @pl.when(z + dist < times)
        def _():
            climb(z + dist, unit).wait_recv()

            @pl.when(z > 0)
            def _():
                descend(z + dist, unit).start()

    halves = steps // 2
    plan = {}
    tail = []
    events = []
    for jb in range(nblocks):
        begin = halves * chips * (jb + 1) + LAG
        events.append((begin, finish, (jb,)))
        for part in range(PARTS):
            for dist in range(1, times):
                at = begin + part + HOP * dist
                events.append((at, relay, (jb * PARTS + part, dist)))
    events.sort(key=lambda event: event[0])
    for at, act, operands in events:
        if at < halves * pieces:
            plan.setdefault(at, []).append((act, operands))
        else:
            tail.append((act, operands))

    def one(piece, carry):
        jb = piece // chips
        s = lax.rem(piece, chips)
        for step in range(0, steps, 2):
            form(lhs_b, piece, step + 1)
            first = product(lhs_a, piece, step)
            acc_ref[...] = first if step == 0 else acc_ref[...] + first
            if step + 2 < steps:
                form(lhs_a, piece, step + 2)
            else:
                form(lhs_a, lax.rem(piece + 1, pieces), 0)
            acc_ref[...] += product(lhs_b, piece, step + 1)
            for at, acts in plan.items():
                if at % halves == step // 2:

                    @pl.when(piece == at // halves)
                    def _():
                        for act, operands in acts:
                            act(*operands)

        @pl.when(s < chips - 1)
        def _():
            send_ref[jb, s] = acc_ref[...].astype(jnp.bfloat16)
            forward(s, jb).start()

        @pl.when(s == chips - 1)
        def _():
            own_ref[jb] = acc_ref[...]

        return carry

    form(lhs_a, 0, 0)
    lax.fori_loop(0, pieces, one, 0)
    for act, operands in tail:
        act(*operands)

    for jb in range(nblocks):
        for s in range(chips - 1):
            forward(s, jb).wait_send()
    for unit in range(nblocks * PARTS):
        for t in range(times):

            @pl.when((z < times - 1) & (t <= z))
            def _():
                climb(t, unit).wait_send()

            @pl.when((z > 0) & (t >= z))
            def _():
                descend(t, unit).wait_send()


def elementals(local, momenta, offsets):
    nvec = local.shape[2]
    sites = local.shape[3]
    groups = lax.axis_size("space")
    times = lax.axis_size("tm")
    chips = groups // 2
    rows = nvec // groups
    moments = momenta.shape[0]
    nblocks = nvec // JB
    group = 2 * moments * JB
    reach = nblocks // 2 + 1
    wide = reach * group
    nchunks = 2 * sites // LANES
    depth = 6 * LANES
    tall = rows * JB
    scale = 1.0 / math.sqrt(sites * groups)
    dma = pltpu.SemaphoreType.DMA
    return pl.pallas_call(
        functools.partial(elementals_kernel, scale, chips, times, rows),
        out_shape=jax.ShapeDtypeStruct(
            (times, nblocks, tall * reach - tall // 2, group), jnp.bfloat16
        ),
        in_specs=[
            pl.BlockSpec(memory_space=pltpu.SMEM),
            pl.BlockSpec(memory_space=pltpu.SMEM),
            pl.BlockSpec(memory_space=pltpu.VMEM),
        ],
        out_specs=pl.BlockSpec(memory_space=pltpu.VMEM),
        scratch_shapes=[
            pltpu.VMEM((2, 3, nvec, sites), jnp.bfloat16),
            pltpu.VMEM((2, 2 * moments, sites), jnp.float32),
            pltpu.VMEM((nchunks, 6, nvec, LANES), jnp.float32),
            pltpu.VMEM(
                (nchunks // SPAN, (nblocks + reach - 1) * group, SPAN * depth), jnp.bfloat16
            ),
            pltpu.VMEM((tall, SPAN * depth), jnp.bfloat16),
            pltpu.VMEM((tall, SPAN * depth), jnp.bfloat16),
            pltpu.VMEM((tall, wide), jnp.float32),
            pltpu.VMEM((nblocks, tall, wide), jnp.float32),
            pltpu.VMEM((nblocks, chips - 1, tall, wide), jnp.bfloat16),
            pltpu.VMEM((nblocks, chips - 1, tall, wide), jnp.bfloat16),
            dma((2,)),
            dma((nblocks, chips - 1)),
            dma((nblocks, chips - 1)),
            dma((nblocks * PARTS, times)),
            dma((nblocks * PARTS, times)),
            dma((nblocks * PARTS, times)),
        ],
        compiler_params=pltpu.CompilerParams(
            collective_id=0, has_side_effects=True, vmem_limit_bytes=60 * 1024 * 1024
        ),
        name="elementals",
    )(momenta, jnp.transpose(offsets), local)


def unpack_kernel(rows, moments, nvec, source, out_ref, grid_ref, place_ref, near_ref, far_ref):
    nblocks = nvec // JB
    group = 2 * moments * JB
    pack = LANES // JB
    wide = 2 * nvec
    tiles = 2 * wide // LANES
    starts = (0, wide // LANES)
    counts = (-(-wide // LANES), tiles - wide // LANES)

    @pl.when(pl.program_id(0) == 0)
    def _():
        for odd in range(2):
            span = counts[odd] * LANES
            shape = (group, moments * span)
            lane = lax.broadcasted_iota(jnp.int32, shape, 0)
            col = lax.broadcasted_iota(jnp.int32, shape, 1)
            which, k = lane // JB, lane % JB
            for kb in range(nblocks):
                goal = which % 2 * nvec + kb * JB + k + odd * wide - starts[odd] * LANES
                hit = which // 2 * span + goal == col
                place_ref[odd, kb * group : (kb + 1) * group, : moments * span] = jnp.where(
                    hit, 1.0, 0.0
                ).astype(jnp.bfloat16)

    reach = nblocks // 2 + 1
    small = JB // 2
    per = rows // PARTS
    slab = per * (reach * JB - small)

    def spot(i, d):
        part, n = divmod(i, per)
        if d == 0:
            return part * slab + per * (reach - 1) * JB + n * small
        return part * slab + (per * (d - 1) + n) * JB

    def take(jb, start, many, d):
        tall = small if d == 0 else JB
        return jnp.concatenate(
            [
                source[0, jb, spot(start + n, d) : spot(start + n, d) + tall, :].astype(jnp.float32)
                for n in range(many)
            ],
            axis=0,
        )

    for jb in range(nblocks):
        for d in range(1, reach):
            kb = (jb + d) % nblocks
            for start in range(0, rows, pack):
                many = min(pack, rows - start)
                block = take(jb, start, many, d)
                turned = -jnp.transpose(block)
                for n in range(many):
                    base = (start + n) * nvec
                    grid_ref[kb, base + jb * JB : base + (jb + 1) * JB, :] = block[
                        n * JB : (n + 1) * JB, :
                    ]
                    for which in range(2 * moments):
                        grid_ref[
                            jb, base + kb * JB : base + (kb + 1) * JB, which * JB : (which + 1) * JB
                        ] = turned[which * JB : (which + 1) * JB, n * JB : (n + 1) * JB]
        for start in range(0, rows, 2 * pack):
            many = min(2 * pack, rows - start)
            block = take(jb, start, many, 0)
            turned = -jnp.transpose(block)
            for n in range(many):
                for which in range(2 * moments):
                    lane = which * JB
                    near = turned[lane : lane + small, n * small : (n + 1) * small]
                    far = turned[lane + small : lane + JB, n * small : (n + 1) * small]
                    near_ref[n * small : (n + 1) * small, lane : lane + small] = near
                    near_ref[n * small : (n + 1) * small, lane + small : lane + JB] = near
                    far_ref[n * small : (n + 1) * small, lane : lane + small] = far
            height = many * small
            j, k = spots(height, group)
            near = near_ref[:height, :]
            top = jnp.where(k > j, block, jnp.where(k < j, near, 0.0))
            lag = k - small
            moved = pltpu.roll(block, small, 1)
            low = jnp.where(lag < j, moved, jnp.where(lag > j, near, 0.0))
            low = jnp.where(k < small, far_ref[:height, :], low)
            for n in range(many):
                base = (start + n) * nvec + jb * JB
                grid_ref[jb, base : base + small, :] = top[n * small : (n + 1) * small, :]
                grid_ref[jb, base + small : base + JB, :] = low[n * small : (n + 1) * small, :]
    lines = rows * nvec // 2
    moved = []
    for odd in range(2):
        taken = [
            grid_ref[kb, pl.ds(odd, lines, stride=2), :].astype(jnp.bfloat16)
            for kb in range(nblocks)
        ]
        moved.append(
            jnp.dot(
                jnp.concatenate(taken, axis=1),
                place_ref[odd, :, : moments * counts[odd] * LANES],
                preferred_element_type=jnp.float32,
            )
        )
    for p in range(moments):
        for tile in range(tiles):
            parts = []
            for odd in range(2):
                n = tile - starts[odd]
                if 0 <= n < counts[odd]:
                    at = (p * counts[odd] + n) * LANES
                    parts.append(moved[odd][:, at : at + LANES])
            out_ref[0, pl.ds(tile * moments + p, lines, stride=tiles * moments), :] = sum(
                parts[1:], parts[0]
            )


def unpack(packed, rows, moments, nvec):
    times = packed.shape[0]
    lines = nvec * nvec * 2 // LANES
    flat = pl.pallas_call(
        functools.partial(unpack_kernel, rows, moments, nvec),
        out_shape=jax.ShapeDtypeStruct((times, rows * lines * moments, LANES), jnp.float32),
        grid=(times,),
        in_specs=[
            pl.BlockSpec((1,) + packed.shape[1:], lambda t: (t, 0, 0, 0)),
        ],
        out_specs=pl.BlockSpec((1, rows * lines * moments, LANES), lambda t: (t, 0, 0)),
        scratch_shapes=[
            pltpu.VMEM((nvec // JB, rows * nvec, LANES), jnp.float32),
            pltpu.VMEM(
                (2, nvec // JB * LANES, moments * -(-2 * nvec // LANES) * LANES), jnp.bfloat16
            ),
            pltpu.VMEM((LANES, LANES), jnp.float32),
            pltpu.VMEM((LANES, LANES), jnp.float32),
        ],
        compiler_params=pltpu.CompilerParams(dimension_semantics=("arbitrary",)),
        name="unpack",
    )(packed)
    flat = flat.reshape(times, rows, lines, moments, LANES)
    return jnp.transpose(flat, (0, 1, 3, 2, 4)).reshape(times, rows, moments, lines * LANES)


def body(vectors, momenta, offsets):
    local = vectors[0]
    nvec = local.shape[2]
    rows = nvec // lax.axis_size("space")
    packed = elementals(local, momenta, offsets)
    return unpack(packed, rows, momenta.shape[0], nvec)


def solution(mesh):
    return jax.shard_map(
        body,
        mesh=mesh,
        in_specs=(P("tm", None, None, None, "space"), P(), P()),
        out_specs=P(None, "space", None, None),
        check_vma=False,
    )
```
